32 devices in a mesh: ga: 2 (over x), row: 8 (over z, y), col: 2 (over core).
Axes of the slice: x: 2, y: 2, z: 4, core: 2. Of those that a mesh axis runs over, the one named last changes fastest.
Arguments:
- pair: bfloat16 [256, 128, 128], P(('ga', 'row', 'col')), parts along dimension 0, may hold values from -480 to 480
- residue_mask: int32 [256], P('ga'), parts along dimension 0, may hold values from 0 to 1, as said below
- targets: int32 [256, 128], P(('ga', 'row', 'col')), parts along dimension 0, may hold values from 0 to 63
- ln_gain: float32 [2, 128], replicated, may hold values from 0.25 to 1.75
- ln_shift: float32 [2, 128], replicated, may hold values from -3 to 3
- w_in: bfloat16 [5, 128, 128], P(None, None, 'col'), may hold values from -0.5 to 0.5
- b_in: float32 [5, 128], replicated, may hold values from -3 to 3
- w_out: bfloat16 [128, 128], P('col'), may hold values from -0.5 to 0.5
- b_out: float32 [128], replicated, may hold values from -3 to 3
- head_weight: bfloat16 [128, 64], replicated, may hold values from -0.5 to 0.5
- head_bias: float32 [64], replicated, may hold values from -4 to 4
Outputs:
- update: bfloat16 [256, 128, 128], P(('ga', 'row', 'col')), parts along dimension 0
- pair_loss: float32 [256, 128], P(('ga', 'row', 'col')), parts along dimension 0
The draws below stay inside these ranges and needn't reach their ends.
There are 2 independent parts, one for each index of `ga`. The reference program is written for one: setup_inputs(seed, part) draws one part's arguments, and reference() takes and returns one part's arrays. A program takes and returns all parts, laid end to end along the dimension named above; an argument that names none is the same for every part. Nothing has to cross between parts.
Inputs may be any that keep to these rules, and one draw needn't show every extreme that they name: `residue_mask`: each part's entries are 1 for residues 0 to some length - 1 and 0 after it; the length is at least 64 and at most 128.
All inputs are finite; a program needn't handle non-finite values.
Results may differ from the reference program's by a relative error of at most 0.0055.
Values may be sent and summed in bfloat16 or wider, within the bound.
A program may use at most 64 MiB of HBM per device.

```python
import jax
import jax.numpy as jnp
from jax import lax

D = 128
BINS = 64
RESIDUES = 128


def draw_pair(key, part):
    first_key, second_key = jax.random.split(key)
    values = jnp.clip(jax.random.normal(first_key, (RESIDUES, RESIDUES, D), jnp.float32), -6.0, 6.0)
    return values.astype(jnp.bfloat16)


def draw_residue_mask(key, part):
    crop_length = jax.random.randint(key, (), RESIDUES // 2, RESIDUES + 1)
    return (jnp.arange(RESIDUES) < crop_length).astype(jnp.int32)


def set_ends(result, key, smallest, largest):
    extent = result.shape
    spot = [jax.random.randint(jax.random.fold_in(key, axis), (), 0, extent[axis]) for axis in range(len(extent))]
    result = result.at[tuple(spot)].set(smallest)
    longest = extent.index(max(extent))
    spot[longest] = (spot[longest] + 1) % extent[longest]
    return result.at[tuple(spot)].set(largest)


def shard_levels(key, dims, pieces, least, high):
    gain, own = 1.0, jax.random.fold_in(key, 6)
    for dim, parts in pieces:
        steps = jnp.exp(jax.random.uniform(jax.random.fold_in(own, dim), (parts,), jnp.float32, least / len(pieces), high / len(pieces)))
        gain = gain * jnp.repeat(steps, dims[dim] // parts).reshape([-1 if axis == dim else 1 for axis in range(len(dims))])
    return gain


def gaussian(own_key, dims, scale, bound, cuts=(), kind=jnp.bfloat16):
    drawn = scale * jax.random.normal(own_key, dims, jnp.float32)
    if cuts:
        drawn = drawn * shard_levels(own_key, dims, cuts, -0.22, 0.18)
    return jnp.clip(drawn, -bound, bound).astype(kind)


def setup_inputs(seed: int = 0, part: int = 0) -> dict:
    key_list = jax.random.split(jax.random.key(seed), 12)
    part_keys = jax.random.split(jax.random.fold_in(key_list[11], part), 12)
    pair = draw_pair(jax.random.fold_in(jax.random.fold_in(key_list[11], part), 71), part)
    residue_mask = draw_residue_mask(jax.random.fold_in(jax.random.fold_in(key_list[11], part), 71), part)
    targets = set_ends(jax.random.randint(part_keys[2], (RESIDUES, RESIDUES), 0, BINS), jax.random.fold_in(part_keys[2], 1), 0, BINS - 1).astype(jnp.int32)
    ln_gain = jnp.clip(1.0 + 0.15 * jax.random.normal(key_list[3], (2, D), jnp.float32), 0.25, 1.75)
    ln_shift = gaussian(key_list[4], (2, D), 0.3, 3.0, (), jnp.float32)
    w_in = gaussian(key_list[5], (5, D, D), D ** -0.5, 0.5, ((2, 2),))
    b_in = gaussian(key_list[6], (5, D), 0.5, 3.0, (), jnp.float32)
    w_out = gaussian(key_list[7], (D, D), D ** -0.5, 0.5, ((0, 2),))
    b_out = gaussian(key_list[8], (D,), 0.5, 3.0, (), jnp.float32)
    head_weight = gaussian(key_list[9], (D, BINS), D ** -0.5, 0.5)
    head_bias = gaussian(key_list[10], (BINS,), 1.0, 4.0, (), jnp.float32)
    return dict(pair=pair, residue_mask=residue_mask, targets=targets, ln_gain=ln_gain, ln_shift=ln_shift, w_in=w_in, b_in=b_in, w_out=w_out, b_out=b_out, head_weight=head_weight, head_bias=head_bias)


def normalize(values, gain_vec, shift_vec, epsilon):
    average = lax.optimization_barrier(jnp.mean(values, axis=-1, keepdims=True))
    centred = values - average
    spread = lax.optimization_barrier(jnp.mean(centred * centred, axis=-1, keepdims=True))
    return centred * lax.rsqrt(spread + epsilon) * gain_vec + shift_vec

def reference(pair, residue_mask, targets, ln_gain, ln_shift, w_in, b_in, w_out, b_out, head_weight, head_bias):
    res_mask = residue_mask.astype(jnp.float32)
    row_block = 32
    block_count = RESIDUES // row_block
    pair_blocks = pair.reshape(block_count, row_block, RESIDUES, D)
    mask_blocks = res_mask.reshape(block_count, row_block)
    weights_in = w_in.astype(jnp.float32)

    def project(operands):
        rows_pair, rows_mask = operands
        normed = normalize(rows_pair.astype(jnp.float32), ln_gain[0], ln_shift[0], 0.1).astype(jnp.bfloat16)
        projected = jnp.einsum('ikc,ncd->nikd', normed.astype(jnp.float32), weights_in) + b_in[:, None, None, :]
        masks = rows_mask[:, None, None] * res_mask[None, :, None]
        left_side = (masks * jax.nn.sigmoid(projected[1]) * projected[0]).astype(jnp.bfloat16)
        right_side = (masks * jax.nn.sigmoid(projected[3]) * projected[2]).astype(jnp.bfloat16)
        gate_value = jax.nn.sigmoid(projected[4])
        return (left_side, right_side, gate_value)
    lefts, rights, gates = lax.map(project, (pair_blocks, mask_blocks))
    left_chan = jnp.transpose(lefts.reshape(RESIDUES, RESIDUES, D), (2, 0, 1))
    right_chan = jnp.transpose(rights.reshape(RESIDUES, RESIDUES, D), (2, 0, 1))

    def triangle(operands):
        left_part, right_part = operands
        product = jnp.einsum('cik,cjk->cij', left_part.astype(jnp.float32), right_part.astype(jnp.float32))
        return product.astype(jnp.bfloat16)
    outer_prod = lax.map(triangle, (left_chan.reshape(D // 8, 8, RESIDUES, RESIDUES), right_chan.reshape(D // 8, 8, RESIDUES, RESIDUES)))
    outer_rows = jnp.transpose(outer_prod.reshape(D, RESIDUES, RESIDUES), (1, 2, 0))
    weights_out = w_out.astype(jnp.float32)
    head_float = head_weight.astype(jnp.float32)

    def finish(operands):
        rows_outer, rows_gate, rows_pair = operands
        normed_outer = normalize(rows_outer.astype(jnp.float32), ln_gain[1], ln_shift[1], 1.0).astype(jnp.bfloat16)
        mixed = jnp.einsum('ijc,cd->ijd', normed_outer.astype(jnp.float32), weights_out) + b_out
        update = (rows_gate * mixed).astype(jnp.bfloat16)
        new_pair = (rows_pair.astype(jnp.float32) + update.astype(jnp.float32)).astype(jnp.bfloat16)
        logits = jnp.einsum('ijc,cb->ijb', new_pair.astype(jnp.float32), head_float) + head_bias
        return (update, logits)
    updates, logit_blocks = lax.map(finish, (outer_rows.reshape(block_count, row_block, RESIDUES, D), gates, pair_blocks))
    update = updates.reshape(RESIDUES, RESIDUES, D)
    logits = logit_blocks.reshape(RESIDUES, RESIDUES, BINS)
    symmetric = logits + jnp.transpose(logits, (1, 0, 2))
    log_total = jax.nn.logsumexp(symmetric, axis=-1)
    picked = jnp.take_along_axis(symmetric, targets[..., None].astype(jnp.int32), axis=-1)[..., 0]
    pair_loss = res_mask[:, None] * res_mask[None, :] * (log_total - picked)
    return (update, pair_loss)
```

```python
import functools

import jax
import jax.numpy as jnp
from jax import lax
from jax.experimental import pallas as pl
from jax.experimental.pallas import tpu as pltpu
from jax.sharding import PartitionSpec as P

SUPER = 2
CHUNKS = 2
F32, BF16 = jnp.float32, jnp.bfloat16
NT = (((1,), (1,)), ((), ()))
TN = (((0,), (0,)), ((), ()))


def dot(lhs, rhs, dims=(((1,), (0,)), ((), ()))):
    return lax.dot_general(lhs, rhs, dims, preferred_element_type=F32)


def kernel(
    rows_n, cols_n, sup, chunks,
    pair, mask, targets, ln_gain, ln_shift, w_in, b_in, w_out, b_out, head_w, head_b,
    update, loss,
    wt, wo, normed, side_f, right_b, left_b, left_in, right_in, prod, outer, outer_f, gate,
    new_pair, logit_b, logit_in, logit_f, own_t,
    w_send, w_recv, l_send, l_recv, r_send, r_recv, o_send, o_recv, m_send, m_recv,
):
    groups = rows_n * cols_n
    count, length, width = pair.shape
    bins = head_w.shape[0]
    per = groups // sup
    share = width // per
    part = share // chunks
    half = w_in.shape[1]
    lanes = 128
    spans = length // lanes
    packed = 128 // bins
    quads = count // packed
    col = lax.axis_index("col")
    me = lax.axis_index("row") * cols_n + col
    block, slot = me // per, me % per

    def where(peer):
        return {"row": peer // cols_n, "col": peer % cols_n}

    def remote(src, dst, send, recv, peer):
        return pltpu.make_async_remote_copy(
            src_ref=src, dst_ref=dst, send_sem=send, recv_sem=recv,
            device_id=where(peer), device_id_type=pl.DeviceIdType.MESH,
        )

    def each(n, body):
        lax.fori_loop(0, n, lambda i, c: (body(i), c)[1], 0)

    barrier = pltpu.get_barrier_semaphore()

    def greet(d):
        pl.semaphore_signal(
            barrier, inc=1, device_id=where((me + 1 + d) % groups),
            device_id_type=pl.DeviceIdType.MESH,
        )

    each(groups - 1, greet)

    mine = pl.ds(pl.multiple_of(col * half, half), half)
    wt[:, mine, :] = w_in[...]
    wo[mine, :] = w_out[...]

    def norm_rows(i):
        values = pair[i].astype(F32)
        centred = values - jnp.mean(values, axis=-1, keepdims=True)
        spread = jnp.mean(centred * centred, axis=-1, keepdims=True)
        scaled = centred * lax.rsqrt(spread + 0.1) * ln_gain[0:1, :] + ln_shift[0:1, :]
        normed[i] = scaled.astype(BF16)

    each(count, norm_rows)

    row_mask = mask[...].astype(F32)
    lane = lax.broadcasted_iota(jnp.int32, (count, length), 1)
    sub = lax.broadcasted_iota(jnp.int32, (count, length), 0)
    own_mask = jnp.sum(jnp.where(lane == me * count + sub, row_mask, 0.0), axis=1, keepdims=True)
    pair_mask = own_mask * row_mask

    small = jnp.concatenate(
        [b_in[...], ln_gain[1:2, :], ln_shift[1:2, :], jnp.zeros((1, width), F32)], axis=0
    ).T

    pl.semaphore_wait(barrier, groups - 1)

    def weight_copies(peer_col):
        peer = me - col + peer_col
        return (
            remote(wt.at[:, mine, :], wt.at[:, mine, :], w_send.at[0, peer_col], w_recv.at[0, col], peer),
            remote(wo.at[mine, :], wo.at[mine, :], w_send.at[1, peer_col], w_recv.at[1, col], peer),
        )

    for d in range(1, cols_n):
        for copy in weight_copies((col + d) % cols_n):
            copy.start()

    def wait_weights(which):
        for d in range(1, cols_n):
            peer_col = (col + d) % cols_n
            theirs = pl.ds(pl.multiple_of(peer_col * half, half), half)
            ref = (wt.at[:, theirs, :], wo.at[theirs, :])[which]
            mine_ref = (wt.at[:, mine, :], wo.at[mine, :])[which]
            peer = me - col + peer_col
            remote(ref, ref, w_send.at[which, peer_col], w_recv.at[which, peer_col], peer).wait_recv()
            remote(mine_ref, mine_ref, w_send.at[which, peer_col], w_recv.at[which, peer_col], peer).wait_send()

    wait_weights(0)

    def make_side(first, out):
        weights = wt[first:first + 2].reshape(2 * width, width)
        value_b, gate_b = small[:, first:first + 1], small[:, first + 1:first + 2]

        for i in range(count):
            both = dot(weights, normed[i], NT)
            value = jax.nn.sigmoid(both[width:] + gate_b) * (both[:width] + value_b)
            for b in range(spans):
                side_f[b, pl.ds(i, width, stride=count), :] = value[:, b * lanes:(b + 1) * lanes]
        for b in range(spans):
            span = slice(b * lanes, (b + 1) * lanes)
            masked = side_f[b].reshape(width, count, lanes) * pair_mask[:, span][None]
            out[:, :, span] = masked.astype(BF16)

    def channels(owner, ch):
        return pl.ds(owner * share + ch * part, part)

    def left_copy(dest, ch):
        return remote(
            left_b.at[channels(dest, ch)],
            left_in.at[pl.ds(ch * part, part), pl.ds(slot * count, count), :],
            l_send.at[ch, dest], l_recv.at[ch, slot], block * per + dest,
        )

    def right_copy(dest, ch):
        return remote(
            right_b.at[channels(dest % per, ch)],
            right_in.at[pl.ds(ch * part, part), pl.ds(me * count, count), :],
            r_send.at[ch, dest], r_recv.at[ch, me], dest,
        )

    def right_local(ch):
        return pltpu.make_async_copy(
            right_b.at[channels(slot, ch)],
            right_in.at[pl.ds(ch * part, part), pl.ds(me * count, count), :],
            r_recv.at[ch, me],
        )

    def left_local(ch):
        return pltpu.make_async_copy(
            left_b.at[channels(slot, ch)],
            left_in.at[pl.ds(ch * part, part), pl.ds(slot * count, count), :],
            l_recv.at[ch, slot],
        )

    def send_right(ch):
        each(groups - 1, lambda d: right_copy((me + 1 + d) % groups, ch).start())
        right_local(ch).start()

    def send_left(ch):
        each(per - 1, lambda d: left_copy((slot + 1 + d) % per, ch).start())
        left_local(ch).start()

    make_side(2, right_b)
    send_right(0)
    make_side(0, left_b)
    send_left(0)
    for ch in range(1, chunks):
        send_right(ch)
        send_left(ch)

    def make_gate(i):
        gate[i] = jax.nn.sigmoid(dot(normed[i], wt[4], NT) + b_in[4:5, :])

    each(count, make_gate)
    wait_weights(1)

    def outer_copy(dest, ch):
        return remote(
            prod.at[pl.ds(ch * part, part), pl.ds(dest * count, count), :],
            outer.at[channels(slot, ch)],
            o_send.at[ch, dest], o_recv.at[ch, slot], block * per + dest,
        )

    def outer_local(ch):
        return pltpu.make_async_copy(
            prod.at[pl.ds(ch * part, part), pl.ds(slot * count, count), :],
            outer.at[channels(slot, ch)],
            o_recv.at[ch, slot],
        )

    for ch in range(chunks):
        def got_left(d):
            source = (slot + 1 + d) % per
            ref = left_in.at[pl.ds(ch * part, part), pl.ds(source * count, count), :]
            remote(ref, ref, l_send.at[ch, source], l_recv.at[ch, source], block * per + source).wait_recv()

        def got_right(d):
            source = (me + 1 + d) % groups
            ref = right_in.at[pl.ds(ch * part, part), pl.ds(source * count, count), :]
            remote(ref, ref, r_send.at[ch, source], r_recv.at[ch, source], source).wait_recv()

        each(per - 1, got_left)
        each(groups - 1, got_right)
        left_local(ch).wait()
        right_local(ch).wait()
        for c in range(ch * part, (ch + 1) * part):
            prod[c] = dot(left_in[c], right_in[c], NT).astype(BF16)
        each(per - 1, lambda d: outer_copy((slot + 1 + d) % per, ch).start())
        outer_local(ch).start()

    for ch in range(chunks):
        def got_outer(d):
            source = (slot + 1 + d) % per
            ref = outer.at[channels(source, ch)]
            remote(ref, ref, o_send.at[ch, source], o_recv.at[ch, source], block * per + source).wait_recv()

        each(per - 1, got_outer)
        outer_local(ch).wait()

    head_t = head_w[...]
    blank = jnp.zeros((bins, width), BF16)
    spread_w = [
        jnp.concatenate([head_t if h == p else blank for h in range(packed)], axis=0)
        for p in range(packed)
    ]
    bias_row = jnp.concatenate([head_b[...]] * packed, axis=1)

    gain_col, shift_col = small[:, 5:6], small[:, 6:7]
    for b in range(spans):
        span = slice(b * lanes, (b + 1) * lanes)
        values = outer[:, :, span].astype(F32)
        average = jnp.sum(values, axis=0) * (1.0 / width)
        outer_f[b] = values.reshape(width * count, lanes)
        centred = values - average[None]
        inverse = lax.rsqrt(jnp.sum(centred * centred, axis=0) * (1.0 / width) + 1.0)
        for i in range(count):
            part_i = outer_f[b, pl.ds(i, width, stride=count), :]
            part_i = (part_i - average[i:i + 1, :]) * inverse[i:i + 1, :] * gain_col + shift_col
            mixed = dot(part_i.astype(BF16), wo[...], TN) + b_out[...]
            rounded = (gate[i, span, :] * mixed).astype(BF16)
            update[i, span, :] = rounded
            new_pair[i, span, :] = (pair[i, span, :].astype(F32) + rounded.astype(F32)).astype(BF16)
    for i in range(quads):
        total = bias_row
        for p in range(packed):
            total = total + dot(new_pair[p * quads + i], spread_w[p], NT)
        logit_b[i] = total.astype(BF16)

    def logit_copy(dest):
        return remote(
            logit_b.at[:, pl.ds(dest * count, count), :], logit_in.at[me],
            m_send.at[dest], m_recv.at[me], dest,
        )

    logit_local = pltpu.make_async_copy(
        logit_b.at[:, pl.ds(me * count, count), :], logit_in.at[me], m_recv.at[me]
    )
    each(groups - 1, lambda d: logit_copy((me + 1 + d) % groups).start())
    logit_local.start()

    bias_col = jnp.concatenate([head_b[...], jnp.zeros((7, bins), F32)], axis=0).T[:, 0:1]
    for i in range(count):
        own_t[i] = dot(head_t, new_pair[i], NT) + bias_col
    at = lax.broadcasted_iota(jnp.int32, (length, length), 0)
    to = lax.broadcasted_iota(jnp.int32, (length, length), 1)
    fold = length // packed
    order = ((at % fold) // quads) * count + (at // fold) * quads + at % quads
    shuffle = jnp.where(order == to, 1.0, 0.0).astype(BF16)

    def got_logit(d):
        source = (me + 1 + d) % groups
        remote(logit_in.at[source], logit_in.at[source], m_send.at[source], m_recv.at[source], source).wait_recv()

    each(groups - 1, got_logit)
    logit_local.wait()
    logit_f[...] = logit_in[...].astype(F32).reshape(logit_f.shape)
    bin_id = lax.broadcasted_iota(jnp.int32, (bins, length), 0)
    for i in range(count):
        flipped = logit_f[pl.ds(i, groups * quads, stride=count), :].T
        flipped = jnp.concatenate([flipped[p * bins:(p + 1) * bins] for p in range(packed)], axis=1)
        symmetric = own_t[i] + dot(flipped.astype(BF16), shuffle)
        top = jnp.max(symmetric, axis=0, keepdims=True)
        total = top + jnp.log(jnp.sum(jnp.exp(symmetric - top), axis=0, keepdims=True))
        chosen = jnp.sum(jnp.where(bin_id == targets[i:i + 1, :], symmetric, 0.0), axis=0, keepdims=True)
        loss[i:i + 1, :] = pair_mask[i:i + 1, :] * (total - chosen)

    for ch in range(chunks):
        each(per - 1, lambda d: left_copy((slot + 1 + d) % per, ch).wait_send())
        each(groups - 1, lambda d: right_copy((me + 1 + d) % groups, ch).wait_send())
        each(per - 1, lambda d: outer_copy((slot + 1 + d) % per, ch).wait_send())
    each(groups - 1, lambda d: logit_copy((me + 1 + d) % groups).wait_send())


def local(rows_n, cols_n, *args):
    pair, residue_mask, targets, ln_gain, ln_shift, w_in, b_in, w_out, b_out, head_w, head_b = args
    count, length, width = pair.shape
    bins = head_w.shape[1]
    groups = rows_n * cols_n
    sup = SUPER
    per = groups // sup
    share = width // per
    chunks = CHUNKS
    packed = 128 // bins
    quads = count // packed
    dma = pltpu.SemaphoreType.DMA
    vmem = pl.BlockSpec(memory_space=pltpu.VMEM)
    return pl.pallas_call(
        functools.partial(kernel, rows_n, cols_n, sup, chunks),
        out_shape=(
            jax.ShapeDtypeStruct(pair.shape, BF16),
            jax.ShapeDtypeStruct((count, length), F32),
        ),
        in_specs=[vmem] * 11,
        out_specs=(vmem, vmem),
        scratch_shapes=[
            pltpu.VMEM((5, width, width), BF16),
            pltpu.VMEM((width, width), BF16),
            pltpu.VMEM((count, length, width), BF16),
            pltpu.VMEM((length // 128, width * count, 128), F32),
            pltpu.VMEM((width, count, length), BF16),
            pltpu.VMEM((width, count, length), BF16),
            pltpu.VMEM((share, per * count, length), BF16),
            pltpu.VMEM((share, length, length), BF16),
            pltpu.VMEM((share, per * count, length), BF16),
            pltpu.VMEM((width, count, length), BF16),
            pltpu.VMEM((length // 128, width * count, 128), F32),
            pltpu.VMEM((count, length, width), F32),
            pltpu.VMEM((count, length, width), BF16),
            pltpu.VMEM((quads, length, 128), BF16),
            pltpu.VMEM((groups, quads, count, 128), BF16),
            pltpu.VMEM((groups * quads * count, 128), F32),
            pltpu.VMEM((count, bins, length), F32),
            dma((2, cols_n)), dma((2, cols_n)),
            dma((chunks, per)), dma((chunks, per)),
            dma((chunks, groups)), dma((chunks, groups)),
            dma((chunks, per)), dma((chunks, per)),
            dma((groups,)), dma((groups,)),
        ],
        compiler_params=pltpu.CompilerParams(
            collective_id=0, has_side_effects=True, vmem_limit_bytes=60 * 1024 * 1024
        ),
    )(
        pair, residue_mask.reshape(1, length), targets, ln_gain, ln_shift,
        jnp.swapaxes(w_in, 1, 2), b_in, w_out, b_out.reshape(1, width), head_w.T, head_b.reshape(1, bins),
    )


def solution(mesh):
    placed = (
        P(("ga", "row", "col"), None, None),
        P("ga"),
        P(("ga", "row", "col"), None),
        P(),
        P(),
        P(None, None, "col"),
        P(),
        P("col", None),
        P(),
        P(),
        P(),
    )
    return jax.shard_map(
        functools.partial(local, mesh.shape["row"], mesh.shape["col"]),
        mesh=mesh,
        in_specs=placed,
        out_specs=(P(("ga", "row", "col"), None, None), P(("ga", "row", "col"), None)),
        check_vma=False,
    )
```

```python
import functools

import jax
import jax.numpy as jnp
from jax import lax
from jax.experimental import pallas as pl
from jax.experimental.pallas import tpu as pltpu
from jax.sharding import PartitionSpec as P

SUPER = 2
CHUNKS = 2
F32, BF16 = jnp.float32, jnp.bfloat16
NT = (((1,), (1,)), ((), ()))
TN = (((0,), (0,)), ((), ()))


def dot(lhs, rhs, dims=(((1,), (0,)), ((), ()))):
    return lax.dot_general(lhs, rhs, dims, preferred_element_type=F32)


def kernel(
    rows_n, cols_n, sup, chunks,
    pair, mask, targets, ln_gain, ln_shift, w_in, b_in, w_out, b_out, head_w, head_b,
    update, loss,
    wt, wo, small, normed, side_f, right_b, left_b, left_in, right_in, prod, outer, outer_f, gate,
    new_pair, logit_b, logit_in, logit_f, own_t,
    w_send, w_recv, l_send, l_recv, r_send, r_recv, o_send, o_recv, m_send, m_recv,
):
    groups = rows_n * cols_n
    count, length, width = pair.shape
    bins = head_w.shape[0]
    per = groups // sup
    share = width // per
    part = share // chunks
    half = w_in.shape[1]
    lanes = 128
    spans = length // lanes
    packed = 128 // bins
    quads = count // packed
    col = lax.axis_index("col")
    me = lax.axis_index("row") * cols_n + col
    block, slot = me // per, me % per

    def where(peer):
        return {"row": peer // cols_n, "col": peer % cols_n}

    def remote(src, dst, send, recv, peer):
        return pltpu.make_async_remote_copy(
            src_ref=src, dst_ref=dst, send_sem=send, recv_sem=recv,
            device_id=where(peer), device_id_type=pl.DeviceIdType.MESH,
        )

    def each(n, body):
        lax.fori_loop(0, n, lambda i, c: (body(i), c)[1], 0, unroll=True)

    barrier = pltpu.get_barrier_semaphore()

    def greet(d):
        pl.semaphore_signal(
            barrier, inc=1, device_id=where((me + 1 + d) % groups),
            device_id_type=pl.DeviceIdType.MESH,
        )

    each(groups - 1, greet)

    mine = pl.ds(pl.multiple_of(col * half, half), half)
    wt[:, mine, :] = w_in[...]
    wo[mine, :] = w_out[...]

    def norm_rows(i):
        values = pair[i].astype(F32)
        centred = values - jnp.mean(values, axis=-1, keepdims=True)
        spread = jnp.mean(centred * centred, axis=-1, keepdims=True)
        scaled = centred * lax.rsqrt(spread + 0.1) * ln_gain[0:1, :] + ln_shift[0:1, :]
        normed[i] = scaled.astype(BF16)

    each(count, norm_rows)

    row_mask = mask[...].astype(F32)
    lane = lax.broadcasted_iota(jnp.int32, (count, length), 1)
    sub = lax.broadcasted_iota(jnp.int32, (count, length), 0)
    own_mask = jnp.sum(jnp.where(lane == me * count + sub, row_mask, 0.0), axis=1, keepdims=True)
    pair_mask = own_mask * row_mask

    small[...] = jnp.concatenate(
        [b_in[...], ln_gain[1:2, :], ln_shift[1:2, :], jnp.zeros((1, width), F32)], axis=0
    ).T

    pl.semaphore_wait(barrier, groups - 1)

    def weight_copies(peer_col):
        peer = me - col + peer_col
        return (
            remote(wt.at[:, mine, :], wt.at[:, mine, :], w_send.at[0, peer_col], w_recv.at[0, col], peer),
            remote(wo.at[mine, :], wo.at[mine, :], w_send.at[1, peer_col], w_recv.at[1, col], peer),
        )

    for d in range(1, cols_n):
        for copy in weight_copies((col + d) % cols_n):
            copy.start()

    def wait_weights(which):
        for d in range(1, cols_n):
            peer_col = (col + d) % cols_n
            theirs = pl.ds(pl.multiple_of(peer_col * half, half), half)
            ref = (wt.at[:, theirs, :], wo.at[theirs, :])[which]
            mine_ref = (wt.at[:, mine, :], wo.at[mine, :])[which]
            peer = me - col + peer_col
            remote(ref, ref, w_send.at[which, peer_col], w_recv.at[which, peer_col], peer).wait_recv()
            remote(mine_ref, mine_ref, w_send.at[which, peer_col], w_recv.at[which, peer_col], peer).wait_send()

    def make_side(first, out, span_w):
        start = pl.multiple_of(span_w * half, half)
        rows = pl.ds(start, half)
        weights = wt[first:first + 2, rows, :].reshape(2 * half, width)
        value_b, gate_b = small[rows, first:first + 1], small[rows, first + 1:first + 2]

        for i in range(count):
            both = dot(weights, normed[i], NT)
            value = jax.nn.sigmoid(both[half:] + gate_b) * (both[:half] + value_b)
            for b in range(spans):
                side_f[b, pl.ds(i, half, stride=count), :] = value[:, b * lanes:(b + 1) * lanes]
        for b in range(spans):
            span = slice(b * lanes, (b + 1) * lanes)
            masked = side_f[b].reshape(half, count, lanes) * pair_mask[:, span][None]
            out[rows, :, span] = masked.astype(BF16)

    def channels(owner, ch):
        return pl.ds(owner * share + ch * part, part)

    def left_copy(dest, ch):
        return remote(
            left_b.at[channels(dest, ch)],
            left_in.at[slot, pl.ds(ch * part, part)],
            l_send.at[ch, dest], l_recv.at[ch, slot], block * per + dest,
        )

    def right_copy(dest, ch):
        return remote(
            right_b.at[channels(dest % per, ch)],
            right_in.at[me, pl.ds(ch * part, part)],
            r_send.at[ch, dest], r_recv.at[ch, me], dest,
        )

    def right_local(ch):
        return pltpu.make_async_copy(
            right_b.at[channels(slot, ch)],
            right_in.at[me, pl.ds(ch * part, part)],
            r_recv.at[ch, me],
        )

    def left_local(ch):
        return pltpu.make_async_copy(
            left_b.at[channels(slot, ch)],
            left_in.at[slot, pl.ds(ch * part, part)],
            l_recv.at[ch, slot],
        )

    quota = per // cols_n

    def send_right(ch, span_w):
        def one(d):
            owner = span_w * quota + (slot + d) % quota
            dest = (block * per + owner + (d // quota) * per) % groups

            @pl.when(dest != me)
            def _():
                right_copy(dest, ch).start()

        each(sup * quota, one)

    def send_left(ch, span_w):
        def one(d):
            owner = span_w * quota + (slot + d) % quota

            @pl.when(owner != slot)
            def _():
                left_copy(owner, ch).start()

        each(quota, one)

    for turn in range(cols_n):
        if turn == 1:
            wait_weights(0)
        span_w = (col + turn) % cols_n
        make_side(2, right_b, span_w)
        send_right(0, span_w)
    right_local(0).start()
    for turn in range(cols_n):
        span_w = (col + turn) % cols_n
        make_side(0, left_b, span_w)
        send_left(0, span_w)
    left_local(0).start()
    for ch in range(1, chunks):
        for turn in range(cols_n):
            send_right(ch, (col + turn) % cols_n)
        right_local(ch).start()
        for turn in range(cols_n):
            send_left(ch, (col + turn) % cols_n)
        left_local(ch).start()

    def make_gate(i):
        gate[i] = jax.nn.sigmoid(dot(normed[i], wt[4], NT) + b_in[4:5, :])

    each(count, make_gate)
    wait_weights(1)

    def outer_copy(dest, ch):
        return remote(
            prod.at[dest, pl.ds(ch * part, part)],
            outer.at[channels(slot, ch)],
            o_send.at[ch, dest], o_recv.at[ch, slot], block * per + dest,
        )

    def outer_local(ch):
        return pltpu.make_async_copy(
            prod.at[slot, pl.ds(ch * part, part)],
            outer.at[channels(slot, ch)],
            o_recv.at[ch, slot],
        )

    for ch in range(chunks):
        def got_left(d):
            source = (slot + 1 + d) % per
            ref = left_in.at[source, pl.ds(ch * part, part)]
            remote(ref, ref, l_send.at[ch, source], l_recv.at[ch, source], block * per + source).wait_recv()

        def got_right(d):
            source = (me + 1 + d) % groups
            ref = right_in.at[source, pl.ds(ch * part, part)]
            remote(ref, ref, r_send.at[ch, source], r_recv.at[ch, source], source).wait_recv()

        each(per - 1, got_left)
        each(groups - 1, got_right)
        left_local(ch).wait()
        right_local(ch).wait()
        for c in range(ch * part, (ch + 1) * part):
            lhs = left_in[:, c].reshape(per * count, length)
            rhs = right_in[:, c].reshape(length, length)
            prod[:, c] = dot(lhs, rhs, NT).astype(BF16).reshape(per, count, length)
        each(per - 1, lambda d: outer_copy((slot + 1 + d) % per, ch).start())
        outer_local(ch).start()

    for ch in range(chunks):
        def got_outer(d):
            source = (slot + 1 + d) % per
            ref = outer.at[channels(source, ch)]
            remote(ref, ref, o_send.at[ch, source], o_recv.at[ch, source], block * per + source).wait_recv()

        each(per - 1, got_outer)
        outer_local(ch).wait()

    head_t = head_w[...]
    blank = jnp.zeros((bins, width), BF16)
    spread_w = [
        jnp.concatenate([head_t if h == p else blank for h in range(packed)], axis=0)
        for p in range(packed)
    ]
    bias_row = jnp.concatenate([head_b[...]] * packed, axis=1)

    gain_col, shift_col = small[:, 5:6], small[:, 6:7]
    for b in range(spans):
        span = slice(b * lanes, (b + 1) * lanes)
        values = outer[:, :, span].astype(F32)
        average = jnp.sum(values, axis=0) * (1.0 / width)
        outer_f[b] = values.reshape(width * count, lanes)
        centred = values - average[None]
        inverse = lax.rsqrt(jnp.sum(centred * centred, axis=0) * (1.0 / width) + 1.0)
        for i in range(count):
            part_i = outer_f[b, pl.ds(i, width, stride=count), :]
            part_i = (part_i - average[i:i + 1, :]) * inverse[i:i + 1, :] * gain_col + shift_col
            mixed = dot(part_i.astype(BF16), wo[...], TN) + b_out[...]
            rounded = (gate[i, span, :] * mixed).astype(BF16)
            update[i, span, :] = rounded
            new_pair[i, span, :] = (pair[i, span, :].astype(F32) + rounded.astype(F32)).astype(BF16)
    for i in range(quads):
        total = bias_row
        for p in range(packed):
            total = total + dot(new_pair[p * quads + i], spread_w[p], NT)
        logit_b[:, i] = total.astype(BF16).reshape(groups, count, 128)

    def logit_copy(dest):
        return remote(
            logit_b.at[dest], logit_in.at[me],
            m_send.at[dest], m_recv.at[me], dest,
        )

    logit_local = pltpu.make_async_copy(
        logit_b.at[me], logit_in.at[me], m_recv.at[me]
    )
    each(groups - 1, lambda d: logit_copy((me + 1 + d) % groups).start())
    logit_local.start()

    bias_col = jnp.concatenate([head_b[...], jnp.zeros((7, bins), F32)], axis=0).T[:, 0:1]
    for i in range(count):
        own_t[i] = dot(head_t, new_pair[i], NT) + bias_col
    at = lax.broadcasted_iota(jnp.int32, (length, length), 0)
    to = lax.broadcasted_iota(jnp.int32, (length, length), 1)
    fold = length // packed
    order = ((at % fold) // quads) * count + (at // fold) * quads + at % quads
    shuffle = jnp.where(order == to, 1.0, 0.0).astype(BF16)

    def got_logit(d):
        source = (me + 1 + d) % groups
        remote(logit_in.at[source], logit_in.at[source], m_send.at[source], m_recv.at[source], source).wait_recv()

    each(groups - 1, got_logit)
    logit_local.wait()
    logit_f[...] = logit_in[...].astype(F32).reshape(logit_f.shape)
    bin_id = lax.broadcasted_iota(jnp.int32, (bins, length), 0)
    for i in range(count):
        flipped = logit_f[pl.ds(i, groups * quads, stride=count), :].T
        flipped = jnp.concatenate([flipped[p * bins:(p + 1) * bins] for p in range(packed)], axis=1)
        symmetric = own_t[i] + dot(flipped.astype(BF16), shuffle)
        top = jnp.max(symmetric, axis=0, keepdims=True)
        total = top + jnp.log(jnp.sum(jnp.exp(symmetric - top), axis=0, keepdims=True))
        chosen = jnp.sum(jnp.where(bin_id == targets[i:i + 1, :], symmetric, 0.0), axis=0, keepdims=True)
        loss[i:i + 1, :] = pair_mask[i:i + 1, :] * (total - chosen)

    for ch in range(chunks):
        each(per - 1, lambda d: left_copy((slot + 1 + d) % per, ch).wait_send())
        each(groups - 1, lambda d: right_copy((me + 1 + d) % groups, ch).wait_send())
        each(per - 1, lambda d: outer_copy((slot + 1 + d) % per, ch).wait_send())
    each(groups - 1, lambda d: logit_copy((me + 1 + d) % groups).wait_send())


def local(rows_n, cols_n, *args):
    pair, residue_mask, targets, ln_gain, ln_shift, w_in, b_in, w_out, b_out, head_w, head_b = args
    count, length, width = pair.shape
    bins = head_w.shape[1]
    groups = rows_n * cols_n
    sup = SUPER
    per = groups // sup
    share = width // per
    chunks = CHUNKS
    packed = 128 // bins
    quads = count // packed
    dma = pltpu.SemaphoreType.DMA
    vmem = pl.BlockSpec(memory_space=pltpu.VMEM)
    return pl.pallas_call(
        functools.partial(kernel, rows_n, cols_n, sup, chunks),
        out_shape=(
            jax.ShapeDtypeStruct(pair.shape, BF16),
            jax.ShapeDtypeStruct((count, length), F32),
        ),
        in_specs=[vmem] * 11,
        out_specs=(vmem, vmem),
        scratch_shapes=[
            pltpu.VMEM((5, width, width), BF16),
            pltpu.VMEM((width, width), BF16),
            pltpu.VMEM((width, 8), F32),
            pltpu.VMEM((count, length, width), BF16),
            pltpu.VMEM((length // 128, width // cols_n * count, 128), F32),
            pltpu.VMEM((width, count, length), BF16),
            pltpu.VMEM((width, count, length), BF16),
            pltpu.VMEM((per, share, count, length), BF16),
            pltpu.VMEM((groups, share, count, length), BF16),
            pltpu.VMEM((per, share, count, length), BF16),
            pltpu.VMEM((width, count, length), BF16),
            pltpu.VMEM((length // 128, width * count, 128), F32),
            pltpu.VMEM((count, length, width), F32),
            pltpu.VMEM((count, length, width), BF16),
            pltpu.VMEM((groups, quads, count, 128), BF16),
            pltpu.VMEM((groups, quads, count, 128), BF16),
            pltpu.VMEM((groups * quads * count, 128), F32),
            pltpu.VMEM((count, bins, length), F32),
            dma((2, cols_n)), dma((2, cols_n)),
            dma((chunks, per)), dma((chunks, per)),
            dma((chunks, groups)), dma((chunks, groups)),
            dma((chunks, per)), dma((chunks, per)),
            dma((groups,)), dma((groups,)),
        ],
        compiler_params=pltpu.CompilerParams(
            collective_id=0, has_side_effects=True, vmem_limit_bytes=60 * 1024 * 1024
        ),
    )(
        pair, residue_mask.reshape(1, length), targets, ln_gain, ln_shift,
        jnp.swapaxes(w_in, 1, 2), b_in, w_out, b_out.reshape(1, width), head_w.T, head_b.reshape(1, bins),
    )


def solution(mesh):
    placed = (
        P(("ga", "row", "col"), None, None),
        P("ga"),
        P(("ga", "row", "col"), None),
        P(),
        P(),
        P(None, None, "col"),
        P(),
        P("col", None),
        P(),
        P(),
        P(),
    )
    return jax.shard_map(
        functools.partial(local, mesh.shape["row"], mesh.shape["col"]),
        mesh=mesh,
        in_specs=placed,
        out_specs=(P(("ga", "row", "col"), None, None), P(("ga", "row", "col"), None)),
        check_vma=False,
    )
```

```python
import functools

import jax
import jax.numpy as jnp
from jax import lax
from jax.experimental import pallas as pl
from jax.experimental.pallas import tpu as pltpu
from jax.sharding import PartitionSpec as P

SUPER = 2
CHUNKS = 2
EIGHTHS = 4
F32, BF16 = jnp.float32, jnp.bfloat16
NT = (((1,), (1,)), ((), ()))
TN = (((0,), (0,)), ((), ()))


def dot(lhs, rhs, dims=(((1,), (0,)), ((), ()))):
    return lax.dot_general(lhs, rhs, dims, preferred_element_type=F32)


def kernel(
    rows_n, cols_n, sup, chunks,
    *refs,
):
    sources, (update_out, loss) = refs[:11], refs[11:13]
    held, rest = refs[13:24], refs[24:]
    (pair, mask, targets, ln_gain, ln_shift, w_in, b_in, w_out, b_out, head_w, head_b) = held
    (
    wt, wo, small, normed, side_f, right_b, left_b, left_in, right_in, prod, outer, outer_f, gate,
        new_pair, logit_b, logit_in, logit_f, own_t,
        w_send, w_recv, l_send, l_recv, r_send, r_recv, o_send, o_recv, m_send, m_recv,
        in_sem, out_sem, update,
    ) = rest
    groups = rows_n * cols_n
    count, length, width = pair.shape
    bins = head_w.shape[0]
    per = groups // sup
    share = width // per
    first = max(share * EIGHTHS // 8, 1)
    edges = [0, first, share] if chunks > 1 else [0, share]
    half = w_in.shape[1]
    lanes = 128
    spans = length // lanes
    packed = 128 // bins
    quads = count // packed
    col = lax.axis_index("col")
    me = lax.axis_index("row") * cols_n + col
    block, slot = lax.div(me, per), lax.rem(me, per)

    def where(peer):
        return {"row": lax.div(peer, cols_n), "col": lax.rem(peer, cols_n)}

    def remote(src, dst, send, recv, peer):
        return pltpu.make_async_remote_copy(
            src_ref=src, dst_ref=dst, send_sem=send, recv_sem=recv,
            device_id=where(peer), device_id_type=pl.DeviceIdType.MESH,
        )

    def each(n, body):
        lax.fori_loop(0, n, lambda i, c: (body(i), c)[1], 0, unroll=True)

    loads = [pltpu.make_async_copy(sources[n], held[n], in_sem.at[n]) for n in range(11)]
    for load in loads:
        load.start()
    barrier = pltpu.get_barrier_semaphore()

    def greet(d):
        pl.semaphore_signal(
            barrier, inc=1, device_id=where(lax.rem(me + 1 + d, groups)),
            device_id_type=pl.DeviceIdType.MESH,
        )

    each(groups - 1, greet)

    def drain(ref, sem):
        pltpu.make_async_copy(ref, ref, sem).wait()


    for load in loads:
        load.wait()
    mine = pl.ds(pl.multiple_of(col * half, half), half)
    wt[:, mine, :] = w_in[...]
    wo[mine, :] = w_out[...]

    def norm_rows(i):
        values = pair[i].astype(F32)
        centred = values - jnp.mean(values, axis=-1, keepdims=True)
        spread = jnp.mean(centred * centred, axis=-1, keepdims=True)
        scaled = centred * lax.rsqrt(spread + 0.1) * ln_gain[0:1, :] + ln_shift[0:1, :]
        normed[i] = scaled.astype(BF16)

    each(count, norm_rows)

    row_mask = mask[...].astype(F32)
    lane = lax.broadcasted_iota(jnp.int32, (count, length), 1)
    sub = lax.broadcasted_iota(jnp.int32, (count, length), 0)
    own_mask = jnp.sum(jnp.where(lane == me * count + sub, row_mask, 0.0), axis=1, keepdims=True)
    pair_mask = own_mask * row_mask

    small[...] = jnp.concatenate(
        [b_in[...], ln_gain[1:2, :], ln_shift[1:2, :], jnp.zeros((1, width), F32)], axis=0
    ).T

    pl.semaphore_wait(barrier, groups - 1)

    def weight_copies(peer_col):
        peer = me - col + peer_col
        return (
            remote(wt.at[:, mine, :], wt.at[:, mine, :], w_send.at[0, peer_col], w_recv.at[0, col], peer),
            remote(wo.at[mine, :], wo.at[mine, :], w_send.at[1, peer_col], w_recv.at[1, col], peer),
        )

    for d in range(1, cols_n):
        for copy in weight_copies(lax.rem(col + d, cols_n)):
            copy.start()

    def wait_weights(which):
        for d in range(1, cols_n):
            peer_col = lax.rem(col + d, cols_n)
            theirs = pl.ds(pl.multiple_of(peer_col * half, half), half)
            ref = (wt.at[:, theirs, :], wo.at[theirs, :])[which]
            mine_ref = (wt.at[:, mine, :], wo.at[mine, :])[which]
            peer = me - col + peer_col
            remote(ref, ref, w_send.at[which, peer_col], w_recv.at[which, peer_col], peer).wait_recv()
            remote(mine_ref, mine_ref, w_send.at[which, peer_col], w_recv.at[which, peer_col], peer).wait_send()

    def make_side(first, out, span_w):
        start = pl.multiple_of(span_w * half, half)
        rows = pl.ds(start, half)
        weights = wt[first:first + 2, rows, :].reshape(2 * half, width)
        value_b, gate_b = small[rows, first:first + 1], small[rows, first + 1:first + 2]

        for i in range(count):
            both = dot(weights, normed[i], NT)
            value = jax.nn.sigmoid(both[half:] + gate_b) * (both[:half] + value_b)
            for b in range(spans):
                side_f[b, pl.ds(i, half, stride=count), :] = value[:, b * lanes:(b + 1) * lanes]
        for b in range(spans):
            span = slice(b * lanes, (b + 1) * lanes)
            masked = side_f[b].reshape(half, count, lanes) * pair_mask[:, span][None]
            out[rows, :, span] = masked.astype(BF16)

    def channels(owner, ch):
        return pl.ds(owner * share + edges[ch], edges[ch + 1] - edges[ch])

    def left_copy(dest, ch):
        return remote(
            left_b.at[channels(dest, ch)],
            left_in.at[slot, pl.ds(edges[ch], edges[ch + 1] - edges[ch])],
            l_send.at[ch], l_recv.at[ch], block * per + dest,
        )

    def right_copy(dest, ch):
        return remote(
            right_b.at[channels(lax.rem(dest, per), ch)],
            right_in.at[me, pl.ds(edges[ch], edges[ch + 1] - edges[ch])],
            r_send.at[ch], r_recv.at[ch], dest,
        )

    def right_local(ch):
        return pltpu.make_async_copy(
            right_b.at[channels(slot, ch)],
            right_in.at[me, pl.ds(edges[ch], edges[ch + 1] - edges[ch])],
            r_recv.at[ch],
        )

    def left_local(ch):
        return pltpu.make_async_copy(
            left_b.at[channels(slot, ch)],
            left_in.at[slot, pl.ds(edges[ch], edges[ch + 1] - edges[ch])],
            l_recv.at[ch],
        )

    quota = per // cols_n

    def send_right(ch, span_w):
        def one(d):
            owner = span_w * quota + lax.rem(slot + d, quota)
            dest = lax.rem(block * per + owner + lax.div(d, quota) * per, groups)

            @pl.when(dest != me)
            def _():
                right_copy(dest, ch).start()

        each(sup * quota, one)

    def send_left(ch, span_w):
        def one(d):
            owner = span_w * quota + lax.rem(slot + d, quota)

            @pl.when(owner != slot)
            def _():
                left_copy(owner, ch).start()

        each(quota, one)

    for turn in range(cols_n):
        if turn == 1:
            wait_weights(0)
        span_w = lax.rem(col + turn, cols_n)
        make_side(2, right_b, span_w)
        send_right(0, span_w)
    right_local(0).start()
    for turn in range(cols_n):
        span_w = lax.rem(col + turn, cols_n)
        make_side(0, left_b, span_w)
        send_left(0, span_w)
    left_local(0).start()
    for ch in range(1, chunks):
        for turn in range(cols_n):
            send_right(ch, lax.rem(col + turn, cols_n))
        right_local(ch).start()
        for turn in range(cols_n):
            send_left(ch, lax.rem(col + turn, cols_n))
        left_local(ch).start()

    def make_gate(i):
        gate[i] = jax.nn.sigmoid(dot(normed[i], wt[4], NT) + b_in[4:5, :])

    each(count, make_gate)
    wait_weights(1)

    def outer_copy(dest, ch):
        return remote(
            prod.at[dest, pl.ds(edges[ch], edges[ch + 1] - edges[ch])],
            outer.at[channels(slot, ch)],
            o_send.at[ch], o_recv.at[ch], block * per + dest,
        )

    def outer_local(ch):
        return pltpu.make_async_copy(
            prod.at[slot, pl.ds(edges[ch], edges[ch + 1] - edges[ch])],
            outer.at[channels(slot, ch)],
            o_recv.at[ch],
        )

    for ch in range(chunks):
        now = pl.ds(edges[ch], edges[ch + 1] - edges[ch])
        drain(left_in.at[:, now], l_recv.at[ch])
        drain(right_in.at[:, now], r_recv.at[ch])
        for c in range(edges[ch], edges[ch + 1]):
            lhs = left_in[:, c].reshape(per * count, length)
            rhs = right_in[:, c].reshape(length, length)
            prod[:, c] = dot(lhs, rhs, NT).astype(BF16).reshape(per, count, length)
        each(per - 1, lambda d: outer_copy(lax.rem(slot + 1 + d, per), ch).start())
        outer_local(ch).start()

    for ch in range(chunks):
        drain(prod.at[:, pl.ds(edges[ch], edges[ch + 1] - edges[ch])], o_recv.at[ch])

    head_t = head_w[...]
    blank = jnp.zeros((bins, width), BF16)
    spread_w = [
        jnp.concatenate([head_t if h == p else blank for h in range(packed)], axis=0)
        for p in range(packed)
    ]
    bias_row = jnp.concatenate([head_b[...]] * packed, axis=1)

    gain_col, shift_col = small[:, 5:6], small[:, 6:7]
    for b in range(spans):
        span = slice(b * lanes, (b + 1) * lanes)
        values = outer[:, :, span].astype(F32)
        average = jnp.sum(values, axis=0) * (1.0 / width)
        outer_f[b] = values.reshape(width * count, lanes)
        centred = values - average[None]
        inverse = lax.rsqrt(jnp.sum(centred * centred, axis=0) * (1.0 / width) + 1.0)
        for i in range(count):
            part_i = outer_f[b, pl.ds(i, width, stride=count), :]
            part_i = (part_i - average[i:i + 1, :]) * inverse[i:i + 1, :] * gain_col + shift_col
            mixed = dot(part_i.astype(BF16), wo[...], TN) + b_out[...]
            rounded = (gate[i, span, :] * mixed).astype(BF16)
            update[i, span, :] = rounded
            new_pair[i, span, :] = (pair[i, span, :].astype(F32) + rounded.astype(F32)).astype(BF16)
    store = pltpu.make_async_copy(update, update_out, out_sem)
    store.start()
    for i in range(quads):
        total = bias_row
        for p in range(packed):
            total = total + dot(new_pair[p * quads + i], spread_w[p], NT)
        logit_b[:, i] = total.astype(BF16).reshape(groups, count, 128)

    def logit_copy(dest):
        return remote(
            logit_b.at[dest], logit_in.at[me],
            m_send.at[0], m_recv.at[0], dest,
        )

    logit_local = pltpu.make_async_copy(
        logit_b.at[me], logit_in.at[me], m_recv.at[0]
    )
    each(groups - 1, lambda d: logit_copy(lax.rem(me + 1 + d, groups)).start())
    logit_local.start()

    bias_col = jnp.concatenate([head_b[...], jnp.zeros((7, bins), F32)], axis=0).T[:, 0:1]
    for i in range(count):
        own_t[i] = dot(head_t, new_pair[i], NT) + bias_col
    at = lax.broadcasted_iota(jnp.int32, (length, length), 0)
    to = lax.broadcasted_iota(jnp.int32, (length, length), 1)
    fold = length // packed
    order = ((at % fold) // quads) * count + (at // fold) * quads + at % quads
    shuffle = jnp.where(order == to, 1.0, 0.0).astype(BF16)

    drain(logit_in, m_recv.at[0])
    logit_f[...] = logit_in[...].astype(F32).reshape(logit_f.shape)
    bin_id = lax.broadcasted_iota(jnp.int32, (bins, length), 0)
    for i in range(count):
        flipped = logit_f[pl.ds(i, groups * quads, stride=count), :].T
        flipped = jnp.concatenate([flipped[p * bins:(p + 1) * bins] for p in range(packed)], axis=1)
        symmetric = own_t[i] + dot(flipped.astype(BF16), shuffle)
        top = jnp.max(symmetric, axis=0, keepdims=True)
        total = top + jnp.log(jnp.sum(jnp.exp(symmetric - top), axis=0, keepdims=True))
        chosen = jnp.sum(jnp.where(bin_id == targets[i:i + 1, :], symmetric, 0.0), axis=0, keepdims=True)
        loss[i:i + 1, :] = pair_mask[i:i + 1, :] * (total - chosen)

    for ch in range(chunks):
        now = pl.ds(edges[ch], edges[ch + 1] - edges[ch])
        drain(left_in.at[pl.ds(0, per - 1), now], l_send.at[ch])
        drain(right_in.at[pl.ds(0, groups - 1), now], r_send.at[ch])
        drain(prod.at[pl.ds(0, per - 1), now], o_send.at[ch])
    drain(logit_in.at[pl.ds(0, groups - 1)], m_send.at[0])
    store.wait()


def local(rows_n, cols_n, *args):
    pair, residue_mask, targets, ln_gain, ln_shift, w_in, b_in, w_out, b_out, head_w, head_b = args
    count, length, width = pair.shape
    bins = head_w.shape[1]
    groups = rows_n * cols_n
    sup = SUPER
    per = groups // sup
    share = width // per
    chunks = CHUNKS
    packed = 128 // bins
    quads = count // packed
    dma = pltpu.SemaphoreType.DMA
    vmem = pl.BlockSpec(memory_space=pltpu.VMEM)
    inputs = (
        pair, residue_mask.reshape(1, length), targets, ln_gain, ln_shift,
        jnp.swapaxes(w_in, 1, 2), b_in, w_out, b_out.reshape(1, width), head_w.T,
        head_b.reshape(1, bins),
    )
    return pl.pallas_call(
        functools.partial(kernel, rows_n, cols_n, sup, chunks),
        out_shape=(
            jax.ShapeDtypeStruct(pair.shape, BF16),
            jax.ShapeDtypeStruct((count, length), F32),
        ),
        in_specs=[pl.BlockSpec(memory_space=pl.ANY)] * 11,
        out_specs=(pl.BlockSpec(memory_space=pl.ANY), vmem),
        scratch_shapes=[pltpu.VMEM(x.shape, x.dtype) for x in inputs] + [
            pltpu.VMEM((5, width, width), BF16),
            pltpu.VMEM((width, width), BF16),
            pltpu.VMEM((width, 8), F32),
            pltpu.VMEM((count, length, width), BF16),
            pltpu.VMEM((length // 128, width // cols_n * count, 128), F32),
            pltpu.VMEM((width, count, length), BF16),
            pltpu.VMEM((width, count, length), BF16),
            pltpu.VMEM((per, share, count, length), BF16),
            pltpu.VMEM((groups, share, count, length), BF16),
            pltpu.VMEM((per, share, count, length), BF16),
            pltpu.VMEM((width, count, length), BF16),
            pltpu.VMEM((length // 128, width * count, 128), F32),
            pltpu.VMEM((count, length, width), F32),
            pltpu.VMEM((count, length, width), BF16),
            pltpu.VMEM((groups, quads, count, 128), BF16),
            pltpu.VMEM((groups, quads, count, 128), BF16),
            pltpu.VMEM((groups * quads * count, 128), F32),
            pltpu.VMEM((count, bins, length), F32),
            dma((2, cols_n)), dma((2, cols_n)),
            dma((chunks,)), dma((chunks,)), dma((chunks,)), dma((chunks,)), dma((chunks,)), dma((chunks,)),
            dma((1,)), dma((1,)),
            dma((11,)), dma, pltpu.VMEM(pair.shape, BF16),
        ],
        compiler_params=pltpu.CompilerParams(
            collective_id=0, has_side_effects=True, vmem_limit_bytes=60 * 1024 * 1024
        ),
    )(*inputs)


def solution(mesh):
    placed = (
        P(("ga", "row", "col"), None, None),
        P("ga"),
        P(("ga", "row", "col"), None),
        P(),
        P(),
        P(None, None, "col"),
        P(),
        P("col", None),
        P(),
        P(),
        P(),
    )
    return jax.shard_map(
        functools.partial(local, mesh.shape["row"], mesh.shape["col"]),
        mesh=mesh,
        in_specs=placed,
        out_specs=(P(("ga", "row", "col"), None, None), P(("ga", "row", "col"), None)),
        check_vma=False,
    )
```

```python
import functools

import jax
import jax.numpy as jnp
from jax import lax
from jax.experimental import pallas as pl
from jax.experimental.pallas import tpu as pltpu
from jax.sharding import PartitionSpec as P

SUPER = 2
CHUNKS = 2
EIGHTHS = 4
F32, BF16 = jnp.float32, jnp.bfloat16
NT = (((1,), (1,)), ((), ()))
TN = (((0,), (0,)), ((), ()))


def dot(lhs, rhs, dims=(((1,), (0,)), ((), ()))):
    return lax.dot_general(lhs, rhs, dims, preferred_element_type=F32)


def kernel(
    rows_n, cols_n, sup, chunks,
    *refs,
):
    sources, (update, loss) = refs[:11], refs[11:13]
    held, rest = refs[13:24], refs[24:]
    (pair, mask, targets, ln_gain, ln_shift, w_in, b_in, w_out, b_out, head_w, head_b) = held
    (
    wt, wo, small, normed, side_f, right_b, left_b, left_in, right_in, prod, outer, outer_f, gate,
        new_pair, logit_b, logit_in, logit_f, own_t,
        w_send, w_recv, l_send, l_recv, r_send, r_recv, o_send, o_recv, m_send, m_recv,
        in_sem,
    ) = rest
    groups = rows_n * cols_n
    count, length, width = pair.shape
    bins = head_w.shape[0]
    per = groups // sup
    share = width // per
    first = max(share * EIGHTHS // 8, 1)
    edges = [0, first, share] if chunks > 1 else [0, share]
    half = w_in.shape[1]
    lanes = 128
    spans = length // lanes
    packed = 128 // bins
    quads = count // packed
    col = lax.axis_index("col")
    me = lax.axis_index("row") * cols_n + col
    block, slot = lax.div(me, per), lax.rem(me, per)

    def where(peer):
        return {"row": lax.div(peer, cols_n), "col": lax.rem(peer, cols_n)}

    def remote(src, dst, send, recv, peer):
        return pltpu.make_async_remote_copy(
            src_ref=src, dst_ref=dst, send_sem=send, recv_sem=recv,
            device_id=where(peer), device_id_type=pl.DeviceIdType.MESH,
        )

    def each(n, body):
        lax.fori_loop(0, n, lambda i, c: (body(i), c)[1], 0, unroll=True)

    loads = [pltpu.make_async_copy(sources[n], held[n], in_sem.at[n]) for n in range(11)]
    for load in loads:
        load.start()
    barrier = pltpu.get_barrier_semaphore()

    def greet(d):
        pl.semaphore_signal(
            barrier, inc=1, device_id=where(lax.rem(me + 1 + d, groups)),
            device_id_type=pl.DeviceIdType.MESH,
        )

    each(groups - 1, greet)

    def drain(ref, sem):
        pltpu.make_async_copy(ref, ref, sem).wait()


    for load in loads:
        load.wait()
    mine = pl.ds(pl.multiple_of(col * half, half), half)
    wt[:, mine, :] = w_in[...]
    wo[mine, :] = w_out[...]

    def norm_rows(i):
        values = pair[i].astype(F32)
        centred = values - jnp.mean(values, axis=-1, keepdims=True)
        spread = jnp.mean(centred * centred, axis=-1, keepdims=True)
        scaled = centred * lax.rsqrt(spread + 0.1) * ln_gain[0:1, :] + ln_shift[0:1, :]
        normed[i] = scaled.astype(BF16)

    each(count, norm_rows)

    row_mask = mask[...].astype(F32)
    lane = lax.broadcasted_iota(jnp.int32, (count, length), 1)
    sub = lax.broadcasted_iota(jnp.int32, (count, length), 0)
    own_mask = jnp.sum(jnp.where(lane == me * count + sub, row_mask, 0.0), axis=1, keepdims=True)
    pair_mask = own_mask * row_mask

    small[...] = jnp.concatenate(
        [b_in[...], ln_gain[1:2, :], ln_shift[1:2, :], jnp.zeros((1, width), F32)], axis=0
    ).T

    pl.semaphore_wait(barrier, groups - 1)

    def weight_copies(peer_col):
        peer = me - col + peer_col
        return (
            remote(wt.at[:, mine, :], wt.at[:, mine, :], w_send.at[0, peer_col], w_recv.at[0, col], peer),
            remote(wo.at[mine, :], wo.at[mine, :], w_send.at[1, peer_col], w_recv.at[1, col], peer),
        )

    for d in range(1, cols_n):
        for copy in weight_copies(lax.rem(col + d, cols_n)):
            copy.start()

    def wait_weights(which):
        for d in range(1, cols_n):
            peer_col = lax.rem(col + d, cols_n)
            theirs = pl.ds(pl.multiple_of(peer_col * half, half), half)
            ref = (wt.at[:, theirs, :], wo.at[theirs, :])[which]
            mine_ref = (wt.at[:, mine, :], wo.at[mine, :])[which]
            peer = me - col + peer_col
            remote(ref, ref, w_send.at[which, peer_col], w_recv.at[which, peer_col], peer).wait_recv()
            remote(mine_ref, mine_ref, w_send.at[which, peer_col], w_recv.at[which, peer_col], peer).wait_send()

    def make_side(first, out, span_w):
        start = pl.multiple_of(span_w * half, half)
        rows = pl.ds(start, half)
        weights = wt[first:first + 2, rows, :].reshape(2 * half, width)
        value_b, gate_b = small[rows, first:first + 1], small[rows, first + 1:first + 2]

        for i in range(count):
            both = dot(weights, normed[i], NT)
            value = jax.nn.sigmoid(both[half:] + gate_b) * (both[:half] + value_b)
            for b in range(spans):
                side_f[b, pl.ds(i, half, stride=count), :] = value[:, b * lanes:(b + 1) * lanes]
        for b in range(spans):
            span = slice(b * lanes, (b + 1) * lanes)
            masked = side_f[b].reshape(half, count, lanes) * pair_mask[:, span][None]
            out[rows, :, span] = masked.astype(BF16)

    def channels(owner, ch):
        return pl.ds(owner * share + edges[ch], edges[ch + 1] - edges[ch])

    def left_copy(dest, ch):
        return remote(
            left_b.at[channels(dest, ch)],
            left_in.at[slot, pl.ds(edges[ch], edges[ch + 1] - edges[ch])],
            l_send.at[ch], l_recv.at[ch], block * per + dest,
        )

    def right_copy(dest, ch):
        return remote(
            right_b.at[channels(lax.rem(dest, per), ch)],
            right_in.at[me, pl.ds(edges[ch], edges[ch + 1] - edges[ch])],
            r_send.at[ch], r_recv.at[ch], dest,
        )

    def right_local(ch):
        return pltpu.make_async_copy(
            right_b.at[channels(slot, ch)],
            right_in.at[me, pl.ds(edges[ch], edges[ch + 1] - edges[ch])],
            r_recv.at[ch],
        )

    def left_local(ch):
        return pltpu.make_async_copy(
            left_b.at[channels(slot, ch)],
            left_in.at[slot, pl.ds(edges[ch], edges[ch + 1] - edges[ch])],
            l_recv.at[ch],
        )

    quota = per // cols_n

    def send_right(ch, span_w):
        def one(d):
            owner = span_w * quota + lax.rem(slot + d, quota)
            dest = lax.rem(block * per + owner + lax.div(d, quota) * per, groups)

            @pl.when(dest != me)
            def _():
                right_copy(dest, ch).start()

        each(sup * quota, one)

    def send_left(ch, span_w):
        def one(d):
            owner = span_w * quota + lax.rem(slot + d, quota)

            @pl.when(owner != slot)
            def _():
                left_copy(owner, ch).start()

        each(quota, one)

    for turn in range(cols_n):
        if turn == 1:
            wait_weights(0)
        span_w = lax.rem(col + turn, cols_n)
        make_side(2, right_b, span_w)
        send_right(0, span_w)
    right_local(0).start()
    for turn in range(cols_n):
        span_w = lax.rem(col + turn, cols_n)
        make_side(0, left_b, span_w)
        send_left(0, span_w)
    left_local(0).start()
    for ch in range(1, chunks):
        for turn in range(cols_n):
            send_right(ch, lax.rem(col + turn, cols_n))
        right_local(ch).start()
        for turn in range(cols_n):
            send_left(ch, lax.rem(col + turn, cols_n))
        left_local(ch).start()

    def make_gate(i):
        gate[i] = jax.nn.sigmoid(dot(normed[i], wt[4], NT) + b_in[4:5, :])

    each(count, make_gate)
    wait_weights(1)

    def outer_copy(dest, ch):
        return remote(
            prod.at[dest, pl.ds(edges[ch], edges[ch + 1] - edges[ch])],
            outer.at[channels(slot, ch)],
            o_send.at[ch], o_recv.at[ch], block * per + dest,
        )

    def outer_local(ch):
        return pltpu.make_async_copy(
            prod.at[slot, pl.ds(edges[ch], edges[ch + 1] - edges[ch])],
            outer.at[channels(slot, ch)],
            o_recv.at[ch],
        )

    for ch in range(chunks):
        now = pl.ds(edges[ch], edges[ch + 1] - edges[ch])
        drain(left_in.at[:, now], l_recv.at[ch])
        drain(right_in.at[:, now], r_recv.at[ch])
        for c in range(edges[ch], edges[ch + 1]):
            lhs = left_in[:, c].reshape(per * count, length)
            rhs = right_in[:, c].reshape(length, length)
            prod[:, c] = dot(lhs, rhs, NT).astype(BF16).reshape(per, count, length)
        each(per - 1, lambda d: outer_copy(lax.rem(slot + 1 + d, per), ch).start())
        outer_local(ch).start()

    for ch in range(chunks):
        drain(prod.at[:, pl.ds(edges[ch], edges[ch + 1] - edges[ch])], o_recv.at[ch])

    head_t = head_w[...]
    blank = jnp.zeros((bins, width), BF16)
    spread_w = [
        jnp.concatenate([head_t if h == p else blank for h in range(packed)], axis=0)
        for p in range(packed)
    ]
    bias_row = jnp.concatenate([head_b[...]] * packed, axis=1)

    gain_col, shift_col = small[:, 5:6], small[:, 6:7]
    for b in range(spans):
        span = slice(b * lanes, (b + 1) * lanes)
        values = outer[:, :, span].astype(F32)
        average = jnp.sum(values, axis=0) * (1.0 / width)
        outer_f[b] = values.reshape(width * count, lanes)
        centred = values - average[None]
        inverse = lax.rsqrt(jnp.sum(centred * centred, axis=0) * (1.0 / width) + 1.0)
        for i in range(count):
            part_i = outer_f[b, pl.ds(i, width, stride=count), :]
            part_i = (part_i - average[i:i + 1, :]) * inverse[i:i + 1, :] * gain_col + shift_col
            mixed = dot(part_i.astype(BF16), wo[...], TN) + b_out[...]
            rounded = (gate[i, span, :] * mixed).astype(BF16)
            update[i, span, :] = rounded
            new_pair[i, span, :] = (pair[i, span, :].astype(F32) + rounded.astype(F32)).astype(BF16)
    for i in range(quads):
        total = bias_row
        for p in range(packed):
            total = total + dot(new_pair[p * quads + i], spread_w[p], NT)
        logit_b[:, i] = total.astype(BF16).reshape(groups, count, 128)

    def logit_copy(dest):
        return remote(
            logit_b.at[dest], logit_in.at[me],
            m_send.at[0], m_recv.at[0], dest,
        )

    logit_local = pltpu.make_async_copy(
        logit_b.at[me], logit_in.at[me], m_recv.at[0]
    )
    each(groups - 1, lambda d: logit_copy(lax.rem(me + 1 + d, groups)).start())
    logit_local.start()

    bias_col = jnp.concatenate([head_b[...], jnp.zeros((7, bins), F32)], axis=0).T[:, 0:1]
    for i in range(count):
        own_t[i] = dot(head_t, new_pair[i], NT) + bias_col
    at = lax.broadcasted_iota(jnp.int32, (length, length), 0)
    to = lax.broadcasted_iota(jnp.int32, (length, length), 1)
    fold = length // packed
    order = ((at % fold) // quads) * count + (at // fold) * quads + at % quads
    shuffle = jnp.where(order == to, 1.0, 0.0).astype(BF16)

    drain(logit_in, m_recv.at[0])
    logit_f[...] = logit_in[...].astype(F32).reshape(logit_f.shape)
    bin_id = lax.broadcasted_iota(jnp.int32, (bins, length), 0)
    for i in range(count):
        flipped = logit_f[pl.ds(i, groups * quads, stride=count), :].T
        flipped = jnp.concatenate([flipped[p * bins:(p + 1) * bins] for p in range(packed)], axis=1)
        symmetric = own_t[i] + dot(flipped.astype(BF16), shuffle)
        top = jnp.max(symmetric, axis=0, keepdims=True)
        total = top + jnp.log(jnp.sum(jnp.exp(symmetric - top), axis=0, keepdims=True))
        chosen = jnp.sum(jnp.where(bin_id == targets[i:i + 1, :], symmetric, 0.0), axis=0, keepdims=True)
        loss[i:i + 1, :] = pair_mask[i:i + 1, :] * (total - chosen)

    for ch in range(chunks):
        now = pl.ds(edges[ch], edges[ch + 1] - edges[ch])
        drain(left_in.at[pl.ds(0, per - 1), now], l_send.at[ch])
        drain(right_in.at[pl.ds(0, groups - 1), now], r_send.at[ch])
        drain(prod.at[pl.ds(0, per - 1), now], o_send.at[ch])
    drain(logit_in.at[pl.ds(0, groups - 1)], m_send.at[0])


def local(rows_n, cols_n, *args):
    pair, residue_mask, targets, ln_gain, ln_shift, w_in, b_in, w_out, b_out, head_w, head_b = args
    count, length, width = pair.shape
    bins = head_w.shape[1]
    groups = rows_n * cols_n
    sup = SUPER
    per = groups // sup
    share = width // per
    chunks = CHUNKS
    packed = 128 // bins
    quads = count // packed
    dma = pltpu.SemaphoreType.DMA
    vmem = pl.BlockSpec(memory_space=pltpu.VMEM)
    inputs = (
        pair, residue_mask.reshape(1, length), targets, ln_gain, ln_shift,
        jnp.swapaxes(w_in, 1, 2), b_in, w_out, b_out.reshape(1, width), head_w.T,
        head_b.reshape(1, bins),
    )
    return pl.pallas_call(
        functools.partial(kernel, rows_n, cols_n, sup, chunks),
        out_shape=(
            pltpu.VMEM(pair.shape, BF16),
            pltpu.VMEM((count, length), F32),
        ),
        in_specs=[pl.BlockSpec(memory_space=pl.ANY)] * 11,
        out_specs=(vmem, vmem),
        scratch_shapes=[pltpu.VMEM(x.shape, x.dtype) for x in inputs] + [
            pltpu.VMEM((5, width, width), BF16),
            pltpu.VMEM((width, width), BF16),
            pltpu.VMEM((width, 8), F32),
            pltpu.VMEM((count, length, width), BF16),
            pltpu.VMEM((length // 128, width // cols_n * count, 128), F32),
            pltpu.VMEM((width, count, length), BF16),
            pltpu.VMEM((width, count, length), BF16),
            pltpu.VMEM((per, share, count, length), BF16),
            pltpu.VMEM((groups, share, count, length), BF16),
            pltpu.VMEM((per, share, count, length), BF16),
            pltpu.VMEM((width, count, length), BF16),
            pltpu.VMEM((length // 128, width * count, 128), F32),
            pltpu.VMEM((count, length, width), F32),
            pltpu.VMEM((count, length, width), BF16),
            pltpu.VMEM((groups, quads, count, 128), BF16),
            pltpu.VMEM((groups, quads, count, 128), BF16),
            pltpu.VMEM((groups * quads * count, 128), F32),
            pltpu.VMEM((count, bins, length), F32),
            dma((2, cols_n)), dma((2, cols_n)),
            dma((chunks,)), dma((chunks,)), dma((chunks,)), dma((chunks,)), dma((chunks,)), dma((chunks,)),
            dma((1,)), dma((1,)),
            dma((11,)),
        ],
        compiler_params=pltpu.CompilerParams(
            collective_id=0, has_side_effects=True, vmem_limit_bytes=60 * 1024 * 1024
        ),
    )(*inputs)


def solution(mesh):
    placed = (
        P(("ga", "row", "col"), None, None),
        P("ga"),
        P(("ga", "row", "col"), None),
        P(),
        P(),
        P(None, None, "col"),
        P(),
        P("col", None),
        P(),
        P(),
        P(),
    )
    return jax.shard_map(
        functools.partial(local, mesh.shape["row"], mesh.shape["col"]),
        mesh=mesh,
        in_specs=placed,
        out_specs=(P(("ga", "row", "col"), None, None), P(("ga", "row", "col"), None)),
        check_vma=False,
    )
```
